32 devices in a mesh: expert: 8 (over z, y), tensor: 4 (over x, core).
Axes of the slice: x: 2, y: 2, z: 4, core: 2. Of those that a mesh axis runs over, the one named last changes fastest.
Arguments:
- tokens: bfloat16 [1024, 2880], P(('expert', 'tensor')), may hold values from -6 to 6
- cotangent: bfloat16 [1024, 2880], P(('expert', 'tensor')), may hold values from -6 to 6
- routes: int32 [1024, 4], P(('expert', 'tensor')), may hold values from 0 to 7, all different within a row; in each aligned block of 32 rows (0 to 31, 32 to 63, ...) at most 24 rows name the same one
- combine: float32 [1024, 4], P(('expert', 'tensor')), may hold values from 0.1 to 1
- w_gate: bfloat16 [8, 2880, 1440], P('expert', None, 'tensor'), may hold values from -0.109375 to 0.109375
- w_up: bfloat16 [8, 2880, 1440], P('expert', None, 'tensor'), may hold values from -0.109375 to 0.109375
- w_down: bfloat16 [8, 1440, 2880], P('expert', 'tensor'), may hold values from -0.15625 to 0.15625
Outputs:
- token_grad: bfloat16 [1024, 2880], P(('expert', 'tensor'))
- gate_grad: bfloat16 [8, 2880, 1440], P('expert', None, 'tensor')
- up_grad: bfloat16 [8, 2880, 1440], P('expert', None, 'tensor')
- down_grad: bfloat16 [8, 1440, 2880], P('expert', 'tensor')
The draws below stay inside these ranges and needn't reach their ends.
Inputs may be any that keep to these rules, and one draw needn't show every extreme that they name: `routes`: each row names 4 different experts. Among the rows of one device no expert is named more than 24 times, and in every draw some expert is named exactly 24 times by the rows of some device.
All inputs are finite; a program needn't handle non-finite values.
Results may differ from the reference program's by a relative error of at most 0.0065.
Values may be sent and summed in bfloat16 or wider, within the bound.
A program may use at most 128 MiB of HBM per device.

```python
import math
import jax
import jax.numpy as jnp
import numpy as np
from jax import lax

D = 2880
H = 1440
TOP = 4
TOK_DEV = 32
EXPERTS = 8
CAP = 24
TOKENS = 1024
N_EXPERT = 8
N_TENSOR = 4


def levels(stream_key, shape, shards, smallest, top_value):
    level, own = 1.0, jax.random.fold_in(stream_key, 6)
    for position, shards_of in shards:
        steps = jnp.exp(jax.random.uniform(jax.random.fold_in(own, position), (shards_of,), jnp.float32, smallest / len(shards), top_value / len(shards)))
        level = level * jnp.repeat(steps, shape[position] // shards_of).reshape([-1 if axis == position else 1 for axis in range(len(shape))])
    return level


def routed_block(stream_key, own, number, rows, count, top, most, lean):
    sequence = jax.random.permutation(stream_key, count)
    packed, common = load_shares(count, rows * top, most, lean, True), load_shares(count, rows * top, most, lean, False)
    places = jnp.arange(count)

    def named(sizes, turn):
        used = int((sizes > 0).sum())
        fixed = max(1, used // 4)
        moved = fixed + (places - fixed + turn * (used - fixed)) % max(1, count - fixed)
        return jnp.zeros((count,), jnp.int32).at[sequence[jnp.where(places < fixed, places, moved)]].set(jnp.asarray(sizes, jnp.int32))

    sizes = jnp.where(number % 4 == 0, named(packed, number // 4), named(common, number - number // 4 - 1))
    mixed = jax.random.permutation(jax.random.fold_in(own, 3), count)
    giver, sink = mixed[0:count // 2 * 2:2], mixed[1:count // 2 * 2:2]
    slack = jnp.minimum(sizes[giver] - 1, most - sizes[sink]) // 2
    slack = jnp.where((giver == sequence[0]) | (sink == sequence[0]) | (sizes[sink] == 0), 0, jnp.maximum(slack, 0))
    moved = jax.random.randint(jax.random.fold_in(own, 4), (count // 2,), 0, 1 << 20) % (slack + 1)
    sizes = sizes.at[giver].add(-moved).at[sink].add(moved)
    items = jnp.searchsorted(jnp.cumsum(sizes), jnp.arange(rows * top), side="right").astype(jnp.int32)
    grid = items.reshape(top, rows).T
    grid = grid[jax.random.permutation(jax.random.fold_in(own, 1), rows)]
    turn = jax.random.randint(jax.random.fold_in(own, 2), (rows, 1), 0, top)
    return jnp.take_along_axis(grid, (jnp.arange(top)[None, :] + turn) % top, axis=1)


def load_shares(amount, total, most, lean, full):
    weights = [(1 << 20) // math.isqrt(standing ** lean) + 1 for standing in range(1, amount + 1)]
    largest = most if full else min(most, max(-(-total // amount), total * weights[0] // sum(weights)))
    least = 1 if total - largest >= amount - 1 else 0
    given, spare = [largest] + [least] * (amount - 1), total - largest - least * (amount - 1)
    while spare > 0:
        free = [i for i in range(1, amount) if given[i] < largest] or [i for i in range(1, amount) if given[i] < most]
        mass, remaining = sum([weights[i] for i in free]), spare
        for i in free:
            more = min(most - given[i], max(1, remaining * weights[i] // mass), spare)
            given[i] = given[i] + more
            spare = spare - more
    return np.array(given)


def centred(own_key, shape, deviation, bound, cuts=(), kind=jnp.bfloat16):
    factor_of = levels(own_key, shape, cuts, -0.22, 0.18) if cuts else 1.0
    array = jax.random.normal(own_key, shape, jnp.float32) * deviation * factor_of
    return jnp.minimum(jnp.maximum(array, -bound), bound).astype(kind)


def setup_inputs(seed: int = 0) -> dict:
    key_of = jax.random.split(jax.random.key(seed), 8)
    tokens = centred(key_of[0], (TOKENS, D), 1.0, 6.0, ((0, 32),))
    cotangent = centred(key_of[1], (TOKENS, D), 1.0, 6.0, ((0, 32),))
    routes_keys = jax.random.split(jax.random.fold_in(key_of[2], 1), TOKENS // TOK_DEV)
    routes_turns = jax.random.permutation(jax.random.fold_in(key_of[2], 3), TOKENS // TOK_DEV)
    routes = jax.vmap(lambda own, number: routed_block(jax.random.fold_in(key_of[2], 2), own, number, TOK_DEV, EXPERTS, TOP, CAP, 2))(routes_keys, routes_turns).reshape((TOKENS, TOP))
    combine = jnp.clip(jnp.exp(math.log(1.0) - 2.3025851 * jax.random.uniform(key_of[3], (TOKENS, TOP), jnp.float32) ** levels(key_of[3], (TOKENS, TOP), ((0, 32),), -0.2, 0.2)), 0.1, 1.0)
    w_gate = centred(key_of[4], (EXPERTS, D, H), D ** -0.5, 0.109375, ((0, 8), (2, 4)))
    w_up = centred(key_of[5], (EXPERTS, D, H), D ** -0.5, 0.109375, ((0, 8), (2, 4)))
    w_down = centred(key_of[6], (EXPERTS, H, D), H ** -0.5, 0.15625, ((0, 8), (1, 4)))
    return {"tokens": tokens, "cotangent": cotangent, "routes": routes, "combine": combine, "w_gate": w_gate, "w_up": w_up, "w_down": w_down}


def route_slots(flat, experts, cap):
    onehot = (flat[:, None] == jnp.arange(experts, dtype=jnp.int32)[None, :]).astype(jnp.int32)
    before = jnp.cumsum(onehot, axis=0) - onehot
    place = jnp.sum(before * onehot, axis=1)
    return (flat * cap + place).astype(jnp.int32)


def slot_sources(slot, count):
    target = jnp.arange(count, dtype=jnp.int32)
    match = slot[None, :] == target[:, None]
    valid = jnp.any(match, axis=1)
    order = jnp.arange(slot.shape[0], dtype=jnp.int32)
    source = jnp.sum(jnp.where(match, order[None, :], 0), axis=1).astype(jnp.int32)
    return source, valid


def reference(tokens, cotangent, routes, combine, w_gate, w_up, w_down):
    devices = N_EXPERT * N_TENSOR
    per_dev = TOK_DEV * TOP
    flat = routes.reshape(devices, per_dev).astype(jnp.int32)
    slots = jax.vmap(lambda f: route_slots(f, EXPERTS, CAP))(flat)
    source, valid = jax.vmap(lambda s: slot_sources(s, EXPERTS * CAP))(slots)
    offset = jnp.arange(devices, dtype=jnp.int32)[:, None] * per_dev
    route_index = (source + offset).astype(jnp.int32)
    route_index = route_index.reshape(devices, EXPERTS, CAP).transpose(1, 0, 2).reshape(EXPERTS, devices * CAP)
    valid = valid.reshape(devices, EXPERTS, CAP).transpose(1, 0, 2).reshape(EXPERTS, devices * CAP)
    weights_flat = combine.reshape(-1).astype(jnp.float32)

    def expert_step(items):
        e_gate, e_up, e_down, ridx, live = items
        token = (ridx // TOP).astype(jnp.int32)
        xs = jnp.where(live[:, None], tokens[token], 0).astype(tokens.dtype)
        scaled = weights_flat[ridx][:, None] * cotangent[token].astype(jnp.float32)
        dys = jnp.where(live[:, None], scaled, 0.0).astype(jnp.bfloat16)
        gate = jnp.dot(xs, e_gate, preferred_element_type=jnp.float32)
        upper = jnp.dot(xs, e_up, preferred_element_type=jnp.float32)
        sigma = jax.nn.sigmoid(gate)
        act = (gate * sigma * upper).astype(jnp.bfloat16)
        d_act = jnp.dot(dys, e_down.T, preferred_element_type=jnp.float32)
        d_down = jnp.dot(act.T, dys, preferred_element_type=jnp.float32).astype(jnp.bfloat16)
        d_upper = (d_act * gate * sigma).astype(jnp.bfloat16)
        d_gate = (d_act * upper * sigma * (1.0 + gate * (1.0 - sigma))).astype(jnp.bfloat16)
        g_grad = jnp.dot(xs.T, d_gate, preferred_element_type=jnp.float32).astype(jnp.bfloat16)
        u_grad = jnp.dot(xs.T, d_upper, preferred_element_type=jnp.float32).astype(jnp.bfloat16)
        rows = jnp.dot(d_gate, e_gate.T, preferred_element_type=jnp.float32)
        rows = rows + jnp.dot(d_upper, e_up.T, preferred_element_type=jnp.float32)
        return rows.astype(jnp.bfloat16), g_grad, u_grad, d_down

    dxs, gate_grad, up_grad, down_grad = lax.map(expert_step, (w_gate, w_up, w_down, route_index, valid))
    expert_of = flat
    place = slots - expert_of * CAP
    dev_index = jnp.arange(devices, dtype=jnp.int32)[:, None]
    row_index = (expert_of * (devices * CAP) + dev_index * CAP + place).astype(jnp.int32).reshape(-1)
    picked = dxs.reshape(EXPERTS * devices * CAP, D)[row_index].astype(jnp.float32)
    token_grad = jnp.sum(picked.reshape(TOKENS, TOP, D), axis=1).astype(jnp.bfloat16)
    return token_grad, gate_grad, up_grad, down_grad
```

```python
import jax
import jax.numpy as jnp
from jax import lax
from jax.experimental import pallas as pl
from jax.experimental.pallas import tpu as pltpu
from jax.sharding import PartitionSpec as P

MESH = pl.DeviceIdType.MESH


def route_slots(flat, experts, cap):
    onehot = (flat[:, None] == jnp.arange(experts, dtype=jnp.int32)[None, :]).astype(jnp.int32)
    before = jnp.cumsum(onehot, axis=0) - onehot
    place = jnp.sum(before * onehot, axis=1)
    return flat * cap + place


def contract_rows(left, right):
    return lax.dot_general(
        left, right, (((0,), (0,)), ((), ())), preferred_element_type=jnp.float32
    )


def contract_cols(left, right):
    return lax.dot_general(
        left, right, (((1,), (1,)), ((), ())), preferred_element_type=jnp.float32
    )


def slotted(tokens, cotangent, routes, combine, w_gate, w_up, w_down):
    tok_rows, width = tokens.shape
    top_count = routes.shape[1]
    groups = lax.axis_size("expert")
    experts = groups * w_gate.shape[0]
    cap = max(2, 3 * tok_rows * top_count // (2 * experts))
    flat = routes.reshape(-1)
    slot = route_slots(flat, experts, cap)
    target = jnp.arange(experts * cap, dtype=jnp.int32)
    match = slot[None, :] == target[:, None]
    valid = jnp.any(match, axis=1)
    order = jnp.arange(flat.shape[0], dtype=jnp.int32)
    source = jnp.sum(jnp.where(match, order[None, :], 0), axis=1)
    token = source // top_count
    send_x = jnp.where(valid[:, None], tokens[token], jnp.zeros((), tokens.dtype))
    scaled = combine.reshape(-1)[source][:, None] * cotangent[token].astype(jnp.float32)
    send_dy = jnp.where(valid[:, None], scaled, 0.0).astype(jnp.bfloat16)
    send_x = send_x.reshape(groups, cap, width)
    send_dy = send_dy.reshape(groups, cap, width)
    recv_x, recv_dy = (
        lax.all_to_all(send_x, "expert", split_axis=0, concat_axis=0, tiled=True),
        lax.all_to_all(send_dy, "expert", split_axis=0, concat_axis=0, tiled=True),
    )
    recv_x = recv_x.reshape(groups * cap, width)
    recv_dy = recv_dy.reshape(groups * cap, width)
    xs, dys = (
        lax.all_gather(recv_x, "tensor", axis=0, tiled=True),
        lax.all_gather(recv_dy, "tensor", axis=0, tiled=True),
    )
    gate_w = w_gate[0]
    up_w = w_up[0]
    down_w = w_down[0]
    gate = jnp.dot(xs, gate_w, preferred_element_type=jnp.float32)
    upper = jnp.dot(xs, up_w, preferred_element_type=jnp.float32)
    sigma = jax.nn.sigmoid(gate)
    act = (gate * sigma * upper).astype(jnp.bfloat16)
    d_act = contract_cols(dys, down_w)
    down_grad = contract_rows(act, dys).astype(jnp.bfloat16)
    d_upper = (d_act * gate * sigma).astype(jnp.bfloat16)
    d_gate = (d_act * upper * sigma * (1.0 + gate * (1.0 - sigma))).astype(jnp.bfloat16)
    gate_grad = contract_rows(xs, d_gate).astype(jnp.bfloat16)
    up_grad = contract_rows(xs, d_upper).astype(jnp.bfloat16)
    own = lax.psum_scatter(
        contract_cols(d_gate, gate_w) + contract_cols(d_upper, up_w),
        "tensor",
        scatter_dimension=0,
        tiled=True,
    )
    own = own.astype(jnp.bfloat16).reshape(groups, cap, width)
    back = lax.all_to_all(own, "expert", split_axis=0, concat_axis=0, tiled=True).reshape(
        experts * cap, width
    )
    picked = back[slot].astype(jnp.float32).reshape(tok_rows, top_count, width)
    token_grad = jnp.sum(picked, axis=1).astype(jnp.bfloat16)
    return (token_grad, gate_grad[None], up_grad[None], down_grad[None])


def place():
    e, t = lax.axis_index("expert"), lax.axis_index("tensor")
    return e // 2, lax.rem(e, 2), t // 2, lax.rem(t, 2)


def peers(depth):
    z, y, x, c = place()
    e, t = z * 2 + y, x * 2 + c
    along = [(lax.rem(z + step, depth) * 2 + y, t) for step in range(1, depth)]
    return along, (z * 2 + 1 - y, t), (e, (1 - x) * 2 + c), (e, x * 2 + 1 - c)


def greet(depth):
    along, over_y, over_x, twin = peers(depth)
    barrier = pltpu.get_barrier_semaphore()
    for device in [*along, over_y, over_x, twin]:
        pl.semaphore_signal(barrier, inc=1, device_id=device, device_id_type=MESH)
    pl.semaphore_wait(barrier, depth + 2)


def gather_kernel(depth, s_in, x_in, d_in, s_out, x_out, d_out, send_sem, recv_sem, local_sem):
    z, y, x, c = place()
    along, over_y, over_x, twin = peers(depth)
    ins, outs = (s_in, x_in, d_in), (s_out, x_out, d_out)
    sent = [[], [], []]

    def block(dz, dy, dx, dc=0):
        zz = lax.rem(z + dz, depth)
        yy, xx, cc = (1 - y if dy else y), (1 - x if dx else x), (1 - c if dc else c)
        return (zz * 2 + yy) * 4 + xx * 2 + cc

    def send(p, at, device, first=False):
        copy = pltpu.make_async_remote_copy(
            src_ref=ins[p] if first else outs[p].at[at],
            dst_ref=outs[p].at[at],
            send_sem=send_sem.at[p, len(sent[p])],
            recv_sem=recv_sem.at[p, at],
            device_id=device,
            device_id_type=MESH,
        )
        copy.start()
        sent[p].append(copy)

    def landed(p, at):
        pltpu.make_async_remote_copy(
            src_ref=ins[p],
            dst_ref=outs[p].at[at],
            send_sem=send_sem.at[p, 0],
            recv_sem=recv_sem.at[p, at],
            device_id=twin,
            device_id_type=MESH,
        ).wait_recv()

    me = block(0, 0, 0)
    keep = [pltpu.make_async_copy(ins[p], outs[p].at[me], local_sem.at[p]) for p in range(3)]
    for copy in keep:
        copy.start()
    greet(depth)
    for device in [over_y, over_x, *along, twin]:
        for p in range(3):
            send(p, me, device, True)

    def first_level(dz):
        at = block(dz, 0, 0)
        for p in range(3):
            landed(p, at)
            for device in (over_x, over_y, twin):
                send(p, at, device)

    def second_level(dz):
        by_y, by_x = block(dz, 1, 0), block(dz, 0, 1)
        for p in range(3):
            near, far, onward = (by_x, by_y, over_y) if p == 2 else (by_y, by_x, over_x)
            landed(p, near)
            send(p, near, onward)
            send(p, near, twin)
            landed(p, far)
            send(p, far, twin)

    for dz in range(1, depth):
        first_level(dz)
        second_level(dz - 1)
    second_level(depth - 1)
    for dz in range(depth):
        at = block(dz, 1, 1)
        for p in range(3):
            landed(p, at)
            send(p, at, twin)
    for dz in range(depth):
        for dy in range(2):
            for dx in range(2):
                for p in range(3):
                    landed(p, block(dz, dy, dx, 1))
    for copy in keep:
        copy.wait()
    for p in range(3):
        for copy in sent[p]:
            copy.wait_send()


def gather_all(table, tokens, cotangent):
    count = lax.axis_size("expert") * lax.axis_size("tensor")
    depth = lax.axis_size("expert") // 2
    parts = (table, tokens, cotangent)
    return pl.pallas_call(
        lambda *refs: gather_kernel(depth, *refs),
        out_shape=[jax.ShapeDtypeStruct((count, *a.shape), a.dtype) for a in parts],
        in_specs=[pl.BlockSpec(memory_space=pltpu.VMEM)] * 3,
        out_specs=[pl.BlockSpec(memory_space=pl.ANY)] * 3,
        scratch_shapes=[
            pltpu.SemaphoreType.DMA((3, count - 1)),
            pltpu.SemaphoreType.DMA((3, count)),
            pltpu.SemaphoreType.DMA((3,)),
        ],
        compiler_params=pltpu.CompilerParams(collective_id=0, has_side_effects=True),
    )(*parts)


def scatter_kernel(depth, part, out, total, twin_in, x_in, y_in, z_in, send_sem, recv_sem):
    z, y, x, c = place()
    along, over_y, over_x, twin = peers(depth)
    rows = out.shape[0] // 2
    halves = [pl.ds(0, rows), pl.ds(rows, rows)]
    sent = []

    def block(dz, dy, dx, dc=0):
        zz = lax.rem(z + dz, depth)
        yy, xx, cc = (1 - y if dy else y), (1 - x if dx else x), (1 - c if dc else c)
        return (zz * 2 + yy) * 4 + xx * 2 + cc

    def send(src, dst, device):
        copy = pltpu.make_async_remote_copy(
            src_ref=src,
            dst_ref=dst,
            send_sem=send_sem.at[len(sent)],
            recv_sem=recv_sem.at[len(sent)],
            device_id=device,
            device_id_type=MESH,
        )
        copy.start()
        sent.append(copy)
        return copy

    def add(a, b):
        return (a.astype(jnp.float32) + b.astype(jnp.float32)).astype(jnp.bfloat16)

    steps = [*range(1, depth), 0]
    corners = ((1, 1), (0, 1), (1, 0), (0, 0))
    greet(depth)
    from_twin, over, last, ends = {}, {}, {}, {}
    for dz in steps:
        for dy, dx in corners:
            i = dz * 4 + dy * 2 + dx
            from_twin[i] = send(part.at[block(dz, dy, dx, 1)], twin_in.at[i], twin)

    def merge(half, dz, other):
        over[half, dz, other].wait_recv()
        if half == 0:
            i, got = dz * 4 + other * 2, x_in.at[dz * 2 + other]
        else:
            i, got = dz * 4 + other, y_in.at[dz * 2 + other]
        total[i, halves[half]] = add(total[i, halves[half]], got[...])
        return i

    def first(dz):
        for dy, dx in corners:
            i = dz * 4 + dy * 2 + dx
            from_twin[i].wait_recv()
            total[i] = add(part[block(dz, dy, dx)], twin_in[i])
            if dx:
                over[0, dz, dy] = send(total.at[i, halves[0]], x_in.at[dz * 2 + dy], over_x)
            if dy:
                over[1, dz, dx] = send(total.at[i, halves[1]], y_in.at[dz * 2 + dx], over_y)

    def second(dz):
        i = merge(0, dz, 1)
        last[0, dz] = send(total.at[i, halves[0]], y_in.at[depth * 2 + dz], over_y)
        i = merge(1, dz, 1)
        last[1, dz] = send(total.at[i, halves[1]], x_in.at[depth * 2 + dz], over_x)

    def third(dz):
        for half in range(2):
            i = merge(half, dz, 0)
            last[half, dz].wait_recv()
            got = (x_in if half else y_in)[depth * 2 + dz]
            total[i, halves[half]] = add(total[i, halves[half]], got)
            if dz:
                ends[half, dz] = send(
                    total.at[i, halves[half]], z_in.at[half * (depth - 1) + dz - 1], along[dz - 1]
                )

    for turn in range(depth + 2):
        for stage, lag in ((first, 0), (second, 1), (third, 2)):
            if 0 <= turn - lag < depth:
                stage(steps[turn - lag])
    for half in range(2):
        value = total[0, halves[half]].astype(jnp.float32)
        for dz in range(1, depth):
            ends[half, dz].wait_recv()
            value = value + z_in[half * (depth - 1) + dz - 1].astype(jnp.float32)
        out[halves[half]] = value.astype(jnp.bfloat16)
    for copy in sent:
        copy.wait_send()


def scatter_sum(part, rows):
    width = part.shape[1]
    depth = lax.axis_size("expert") // 2
    copies = depth * 4 + 2 * (depth * 2 + depth + depth - 1)
    half = rows // 2
    return pl.pallas_call(
        lambda *refs: scatter_kernel(depth, *refs),
        out_shape=jax.ShapeDtypeStruct((rows, width), jnp.bfloat16),
        in_specs=[pl.BlockSpec(memory_space=pltpu.VMEM)],
        out_specs=pl.BlockSpec(memory_space=pltpu.VMEM),
        scratch_shapes=[
            pltpu.VMEM((depth * 4, rows, width), jnp.bfloat16),
            pltpu.VMEM((depth * 4, rows, width), jnp.bfloat16),
            pltpu.VMEM((depth * 3, half, width), jnp.bfloat16),
            pltpu.VMEM((depth * 3, half, width), jnp.bfloat16),
            pltpu.VMEM((depth * 2 - 2, half, width), jnp.bfloat16),
            pltpu.SemaphoreType.DMA((copies,)),
            pltpu.SemaphoreType.DMA((copies,)),
        ],
        compiler_params=pltpu.CompilerParams(
            collective_id=1, has_side_effects=True, vmem_limit_bytes=48 * 1024 * 1024
        ),
    )(part.reshape(-1, rows, width))


def dense(tokens, cotangent, routes, combine, w_gate, w_up, w_down):
    rows, width = tokens.shape
    experts = lax.axis_size("expert") * w_gate.shape[0]
    named = routes[:, :, None] == jnp.arange(experts, dtype=jnp.int32)[None, None, :]
    table = jnp.sum(jnp.where(named, combine[:, :, None], 0.0), axis=1).T
    table, xs, cot = gather_all(table, tokens, cotangent)
    xs = xs.reshape(-1, width)
    scale = lax.dynamic_slice_in_dim(table, lax.axis_index("expert"), 1, axis=1).reshape(-1, 1)
    dys = (scale * cot.reshape(-1, width).astype(jnp.float32)).astype(jnp.bfloat16)
    gate_w = w_gate[0]
    up_w = w_up[0]
    down_w = w_down[0]
    gate = jnp.dot(xs, gate_w, preferred_element_type=jnp.float32)
    upper = jnp.dot(xs, up_w, preferred_element_type=jnp.float32)
    sigma = jax.nn.sigmoid(gate)
    act = (gate * sigma * upper).astype(jnp.bfloat16)
    d_act = contract_cols(dys, down_w)
    d_upper = (d_act * gate * sigma).astype(jnp.bfloat16)
    d_gate = (d_act * upper * sigma * (1.0 + gate * (1.0 - sigma))).astype(jnp.bfloat16)
    part = contract_cols(d_gate, gate_w) + contract_cols(d_upper, up_w)
    token_grad = scatter_sum(part.astype(jnp.bfloat16), rows)
    down_grad = contract_rows(act, dys).astype(jnp.bfloat16)
    gate_grad = contract_rows(xs, d_gate).astype(jnp.bfloat16)
    up_grad = contract_rows(xs, d_upper).astype(jnp.bfloat16)
    return (token_grad, gate_grad[None], up_grad[None], down_grad[None])


def on_device(tokens, cotangent, routes, combine, w_gate, w_up, w_down):
    groups, shards = lax.axis_size("expert"), lax.axis_size("tensor")
    rows, top_count = routes.shape
    few = w_gate.shape[0] == 1 and groups <= 2 * top_count
    plan = dense if few and shards == 4 and groups % 2 == 0 and rows % 32 == 0 else slotted
    return plan(tokens, cotangent, routes, combine, w_gate, w_up, w_down)


def solution(mesh):
    in_specs = (
        P(("expert", "tensor"), None),
        P(("expert", "tensor"), None),
        P(("expert", "tensor"), None),
        P(("expert", "tensor"), None),
        P("expert", None, "tensor"),
        P("expert", None, "tensor"),
        P("expert", "tensor", None),
    )
    out_specs = (
        P(("expert", "tensor"), None),
        P("expert", None, "tensor"),
        P("expert", None, "tensor"),
        P("expert", "tensor", None),
    )
    return jax.shard_map(
        on_device, mesh=mesh, in_specs=in_specs, out_specs=out_specs, check_vma=False
    )
```
